16 devices in a mesh: dp: 4 (over z, y), tp: 4 (over x, core).
Axes of the slice: x: 2, y: 2, z: 2, core: 2. Of those that a mesh axis runs over, the one named last changes fastest.
Arguments:
- x_chunk: bfloat16 [16, 1024, 2048], P('dp', 'tp'), parts along dimension 0
- prefix_len: int32 [16], P('dp'), parts along dimension 0
- k_cache: bfloat16 [16, 4096, 16, 128], P('dp', None, 'tp'), parts along dimension 0
- v_cache: bfloat16 [16, 4096, 16, 128], P('dp', None, 'tp'), parts along dimension 0
- ln1_gain: bfloat16 [2048], replicated
- ln1_bias: bfloat16 [2048], replicated
- w_qkv: bfloat16 [2048, 6144], P(None, 'tp')
- b_qkv: bfloat16 [6144], P('tp')
- w_out: bfloat16 [2048, 2048], P('tp')
- b_out: bfloat16 [2048], replicated
- ln2_gain: bfloat16 [2048], replicated
- ln2_bias: bfloat16 [2048], replicated
- w_up: bfloat16 [2048, 8192], P(None, 'tp')
- b_up: bfloat16 [8192], P('tp')
- w_down: bfloat16 [8192, 2048], P('tp')
- b_down: bfloat16 [2048], replicated
Outputs:
- output 1: bfloat16 [16, 1024, 2048], P('dp', 'tp'), parts along dimension 0
- output 2: bfloat16 [16, 4096, 16, 128], P('dp', None, 'tp'), parts along dimension 0
- output 3: bfloat16 [16, 4096, 16, 128], P('dp', None, 'tp'), parts along dimension 0
There are 4 independent parts. The reference program is written for one: setup_inputs(seed, part) draws one part's arguments, and reference() takes and returns one part's arrays. A program takes and returns all parts, laid end to end along the dimension named above; an argument that names none is the same for every part.
All inputs are finite; a program needn't handle non-finite values.
Results may differ from the reference program's by a relative error of at most 0.0119016.
Values are sent between devices in bfloat16 or wider.
A program may use at most 1 GiB of HBM per device.

```python
import jax
import jax.numpy as jnp
from jax import lax

BATCH_SEQS = 4
CHUNK_LEN = 1024
CACHE_LEN = 4096
D_MODEL = 2048
NUM_HEADS = 16
HEAD_DIM = 128
FF_DIM = 4 * D_MODEL
LN_EPS = 1e-5


def setup_inputs(seed: int = 0, part: int = 0) -> dict:
    part_keys = jax.random.split(jax.random.fold_in(jax.random.key(seed), part), 5)
    shared_keys = jax.random.split(jax.random.key(seed + 7919), 12)
    max_start = CACHE_LEN - CHUNK_LEN
    starts = jax.random.randint(part_keys[1], (BATCH_SEQS,), 0, max_start + 1)
    longest = jax.random.randint(part_keys[2], (), 0, BATCH_SEQS)
    prefix_len = jnp.where(jnp.arange(BATCH_SEQS) == longest, max_start, starts).astype(jnp.int32)
    cache_shape = (BATCH_SEQS, CACHE_LEN, NUM_HEADS, HEAD_DIM)
    vec_shape = (D_MODEL,)
    d_scale = D_MODEL ** -0.5

    def normal_draw(key_in, shape_in, std_dev):
        return (std_dev * jax.random.normal(key_in, shape_in, jnp.float32)).astype(jnp.bfloat16)

    def gain_draw(key_in):
        return (1.0 + 0.25 * jax.random.normal(key_in, vec_shape, jnp.float32)).astype(jnp.bfloat16)

    return {
        'x_chunk': normal_draw(part_keys[0], (BATCH_SEQS, CHUNK_LEN, D_MODEL), 1.0),
        'prefix_len': prefix_len,
        'k_cache': normal_draw(part_keys[3], cache_shape, 1.0),
        'v_cache': normal_draw(part_keys[4], cache_shape, 1.0),
        'ln1_gain': gain_draw(shared_keys[0]),
        'ln1_bias': normal_draw(shared_keys[1], vec_shape, 0.25),
        'w_qkv': normal_draw(shared_keys[2], (D_MODEL, 3 * D_MODEL), d_scale),
        'b_qkv': normal_draw(shared_keys[3], (3 * D_MODEL,), 0.25),
        'w_out': normal_draw(shared_keys[4], (D_MODEL, D_MODEL), d_scale),
        'b_out': normal_draw(shared_keys[5], vec_shape, 0.25),
        'ln2_gain': gain_draw(shared_keys[6]),
        'ln2_bias': normal_draw(shared_keys[7], vec_shape, 0.25),
        'w_up': normal_draw(shared_keys[8], (D_MODEL, FF_DIM), d_scale),
        'b_up': normal_draw(shared_keys[9], (FF_DIM,), 0.25),
        'w_down': normal_draw(shared_keys[10], (FF_DIM, D_MODEL), FF_DIM ** -0.5),
        'b_down': normal_draw(shared_keys[11], vec_shape, 0.25),
    }


def layer_norm(tok_rows, ln_gain, ln_bias):
    rows_f32 = tok_rows.astype(jnp.float32)
    row_mean = jnp.mean(rows_f32, axis=-1, keepdims=True)
    centered = rows_f32 - row_mean
    row_var = jnp.mean(centered * centered, axis=-1, keepdims=True)
    normed = centered * lax.rsqrt(row_var + LN_EPS)
    return (normed * ln_gain.astype(jnp.float32) + ln_bias.astype(jnp.float32)).astype(jnp.bfloat16)


def write_rows(cache_seq, new_rows, start_pos):
    zero_idx = jnp.zeros_like(start_pos)
    return lax.dynamic_update_slice(cache_seq, new_rows, (start_pos, zero_idx, zero_idx))


def attend_one(operands):
    queries, keys_all, values_all, start_pos = operands
    scores = jnp.einsum('chd,thd->hct', queries.astype(jnp.float32), keys_all.astype(jnp.float32)) * (HEAD_DIM ** -0.5)
    slopes = jnp.exp2(-8.0 * (jnp.arange(NUM_HEADS) + 1).astype(jnp.float32) / NUM_HEADS)
    query_pos = start_pos + jnp.arange(CHUNK_LEN)
    rel_pos = (jnp.arange(CACHE_LEN)[None, :] - query_pos[:, None]).astype(jnp.float32)
    scores = scores + slopes[:, None, None] * rel_pos[None]
    scores = jnp.where((rel_pos <= 0.0)[None], scores, -1e30)
    attn_probs = jax.nn.softmax(scores, axis=-1).astype(jnp.bfloat16)
    context = jnp.einsum('hct,thd->chd', attn_probs.astype(jnp.float32), values_all.astype(jnp.float32))
    return context.astype(jnp.bfloat16).reshape(CHUNK_LEN, D_MODEL)


def reference(x_chunk, prefix_len, k_cache, v_cache, ln1_gain, ln1_bias, w_qkv, b_qkv, w_out, b_out, ln2_gain, ln2_bias, w_up, b_up, w_down, b_down):
    tok_rows = x_chunk.reshape(BATCH_SEQS * CHUNK_LEN, D_MODEL)
    normed = layer_norm(tok_rows, ln1_gain, ln1_bias)
    qkv_proj = jnp.dot(normed, w_qkv, preferred_element_type=jnp.float32) + b_qkv.astype(jnp.float32)
    qkv_heads = qkv_proj.astype(jnp.bfloat16).reshape(BATCH_SEQS, CHUNK_LEN, NUM_HEADS, 3, HEAD_DIM)
    k_upd = jax.vmap(write_rows)(k_cache, qkv_heads[:, :, :, 1], prefix_len)
    v_upd = jax.vmap(write_rows)(v_cache, qkv_heads[:, :, :, 2], prefix_len)
    context = lax.map(attend_one, (qkv_heads[:, :, :, 0], k_upd, v_upd, prefix_len))
    context = context.reshape(BATCH_SEQS * CHUNK_LEN, D_MODEL)
    attn_out = jnp.dot(context, w_out, preferred_element_type=jnp.float32)
    residual = (tok_rows.astype(jnp.float32) + attn_out + b_out.astype(jnp.float32)).astype(jnp.bfloat16)
    normed2 = layer_norm(residual, ln2_gain, ln2_bias)
    up_pre = jnp.dot(normed2, w_up, preferred_element_type=jnp.float32) + b_up.astype(jnp.float32)
    up_act = jax.nn.gelu(up_pre, approximate=True).astype(jnp.bfloat16)
    down_out = jnp.dot(up_act, w_down, preferred_element_type=jnp.float32)
    x_out = (residual.astype(jnp.float32) + down_out + b_down.astype(jnp.float32)).astype(jnp.bfloat16)
    return x_out.reshape(BATCH_SEQS, CHUNK_LEN, D_MODEL), k_upd, v_upd
```

```python
import functools

import jax
import jax.numpy as jnp
from jax import lax
from jax.experimental import pallas as pl
from jax.experimental.pallas import tpu as pltpu
from jax.sharding import PartitionSpec as P


LN_EPS = 1e-5
LOG2E = 1.4426950408889634
MASKED = -1e30 * LOG2E
F32 = jnp.float32
BF16 = jnp.bfloat16
QB = 512
KB = 512
PREP_TOK = 1024
MLP_ROWS = 512
QKV_GROUP = 2
VMEM_BIG = 60 * 1024 * 1024


def ln_rows(rows, gain, bias):
    rows = rows.astype(F32)
    mean = jnp.mean(rows, axis=-1, keepdims=True)
    centered = rows - mean
    var = jnp.mean(centered * centered, axis=-1, keepdims=True)
    return (centered * lax.rsqrt(var + LN_EPS) * gain + bias).astype(BF16)


def prep_kernel(heads, len_ref, k_ref, v_ref, ko_ref, vo_ref, kt_ref, vt_ref, ks, vs):
    toks = kt_ref.shape[2]
    ko_ref[...] = k_ref[...]
    vo_ref[...] = v_ref[...]

    @pl.when(pl.program_id(1) * toks < len_ref[pl.program_id(0)])
    def _():
        for src, tr, tmp in ((k_ref, kt_ref, ks), (v_ref, vt_ref, vs)):
            tmp[...] = src[0].astype(F32)
            for h in range(heads):
                tr[0, h] = tmp[pl.ds(h, toks, stride=heads), :].astype(BF16)


def prep(lens, kc, vc, heads):
    seqs, rows, hd = kc.shape
    toks = rows // heads
    flat = pl.BlockSpec((1, PREP_TOK * heads, hd), lambda b, j, s: (b, j, 0))
    last = lambda b, s: jnp.maximum((s[b] + PREP_TOK - 1) // PREP_TOK, 1) - 1
    tr = pl.BlockSpec((1, heads, PREP_TOK, hd), lambda b, j, s: (b, 0, jnp.minimum(j, last(b, s)), 0))
    flat_t = jax.ShapeDtypeStruct(kc.shape, BF16)
    tr_t = jax.ShapeDtypeStruct((seqs, heads, toks, hd), BF16)
    return pl.pallas_call(
        functools.partial(prep_kernel, heads),
        grid_spec=pltpu.PrefetchScalarGridSpec(
            num_scalar_prefetch=1,
            grid=(seqs, toks // PREP_TOK),
            in_specs=[flat, flat],
            out_specs=[flat, flat, tr, tr],
            scratch_shapes=[pltpu.VMEM((PREP_TOK * heads, hd), F32)] * 2,
        ),
        out_shape=[flat_t, flat_t, tr_t, tr_t],
        compiler_params=pltpu.CompilerParams(vmem_limit_bytes=VMEM_BIG),
        cost_estimate=pl.CostEstimate(flops=int(2e10), bytes_accessed=kc.size * 12, transcendentals=0),
        name="prep",
    )(lens, kc, vc)


def row_of(ref, n=None):
    vec = ref[...] if n is None else ref[n]
    return vec.astype(F32).reshape(1, -1)


def ln1_kernel(seqs, x_ref, g_ref, lb_ref, bu_ref, up_ref, down_ref, wo_ref, *refs):
    outs, (upq, downq, buf, ub, db, sems, isems, osems) = refs[:seqs], refs[seqs:]
    seq = pl.program_id(0)
    dp = lax.axis_index("dp")
    feats, width = up_ref.shape[0], ub.shape[1]
    few = db.shape[0] - width
    cols = lambda n: pl.ds(pl.multiple_of(dp * n, n), n)
    ins = [pltpu.make_async_copy(up_ref.at[:, cols(width)], ub.at[:feats], isems.at[0]),
           pltpu.make_async_copy(down_ref.at[cols(width)], db.at[:width], isems.at[1]),
           pltpu.make_async_copy(wo_ref.at[cols(few)], db.at[width:], isems.at[2])]
    packs = [pltpu.make_async_copy(ub, upq, osems.at[0]), pltpu.make_async_copy(db, downq, osems.at[1])]

    @pl.when(seq == 0)
    def _():
        for copy in ins:
            copy.start()
        ub[feats:, :] = jnp.broadcast_to(row_of(bu_ref, cols(width)), (ub.shape[0] - feats, width)).astype(BF16)

    normed = ln_rows(x_ref[0], row_of(g_ref), row_of(lb_ref))
    for n in range(seqs):
        @pl.when(seq == n)
        def _(n=n):
            buf[n] = normed
            pltpu.make_async_copy(buf.at[n], outs[n], sems.at[n]).start()

    @pl.when(seq == seqs - 1)
    def _():
        for copy in ins:
            copy.wait()
        for copy in packs:
            copy.start()
        for n in range(seqs):
            pltpu.make_async_copy(buf.at[n], outs[n], sems.at[n]).wait()
        for copy in packs:
            copy.wait()


def ln1(x, g, b, bu, w_up, w_down, w_out, parts):
    seqs, tok, feats = x.shape
    up_t = jax.ShapeDtypeStruct((feats + 16, w_up.shape[1] // parts), BF16)
    down_t = jax.ShapeDtypeStruct(((w_down.shape[0] + w_out.shape[0]) // parts, feats), BF16)
    hbm = pl.BlockSpec(memory_space=pl.ANY)
    return pl.pallas_call(
        functools.partial(ln1_kernel, seqs),
        grid=(seqs,),
        in_specs=[pl.BlockSpec((1, tok, feats), lambda n: (n, 0, 0)), *[pl.BlockSpec(v.shape, lambda n: (0,)) for v in (g, b, bu)], hbm, hbm, hbm],
        out_specs=[hbm] * (seqs + 2),
        out_shape=[jax.ShapeDtypeStruct((tok, feats), BF16)] * seqs + [up_t, down_t],
        scratch_shapes=[pltpu.VMEM((seqs, tok, feats), BF16), pltpu.VMEM(up_t.shape, BF16), pltpu.VMEM(down_t.shape, BF16),
                        pltpu.SemaphoreType.DMA((seqs,)), pltpu.SemaphoreType.DMA((3,)), pltpu.SemaphoreType.DMA((2,))],
        compiler_params=pltpu.CompilerParams(vmem_limit_bytes=VMEM_BIG),
        cost_estimate=pl.CostEstimate(flops=int(2e9), bytes_accessed=x.size * 8, transcendentals=0),
        name="ln1",
    )(x, g, b, bu, w_up, w_down, w_out)


def qkv_kernel(heads, hd, group, idx_ref, p0, p1, p2, p3, w_ref, b_ref,
               q_ref, k_ref, v_ref, ki_ref, vi_ref, norm_s, ks, vs, sems):
    step = pl.program_id(0)
    chunk = norm_s.shape[0]
    toks = chunk // 4

    @pl.when(step == 0)
    def _():
        copies = []
        for n, piece in enumerate((p0, p1, p2, p3)):
            at = pl.ds(pl.multiple_of((idx_ref[0] ^ n) * toks, toks), toks)
            copies.append(pltpu.make_async_copy(piece, norm_s.at[at], sems.at[n]))
        for copy in copies:
            copy.start()
        for copy in copies:
            copy.wait()

    bias = row_of(b_ref)
    bias = jnp.where(step == 0, bias[:, :w_ref.shape[1]], bias[:, w_ref.shape[1]:])
    out = jnp.dot(norm_s[...], w_ref[...], preferred_element_type=F32) + bias
    for n in range(group):
        c0 = n * 3 * hd
        k = out[:, c0 + hd:c0 + 2 * hd]
        v = out[:, c0 + 2 * hd:c0 + 3 * hd]
        q_ref[n] = out[:, c0:c0 + hd].astype(BF16)
        k_ref[n] = k.astype(BF16)
        v_ref[n] = v.astype(BF16)
        ks[pl.ds(step * group + n, chunk, stride=heads), :] = k
        vs[pl.ds(step * group + n, chunk, stride=heads), :] = v

    @pl.when(step == heads // group - 1)
    def _():
        ki_ref[...] = ks[...].astype(BF16)
        vi_ref[...] = vs[...].astype(BF16)


def qkv(idx, pieces, w, b, heads, hd):
    toks, feats = pieces[0].shape
    chunk = toks * len(pieces)
    group = QKV_GROUP
    wide = group * 3 * hd
    hbm = pl.BlockSpec(memory_space=pl.ANY)
    out_h = pl.BlockSpec((group, chunk, hd), lambda n, s: (n, 0, 0))
    out_i = pl.BlockSpec((chunk * heads, hd), lambda n, s: (0, 0))
    h_t = jax.ShapeDtypeStruct((heads, chunk, hd), BF16)
    i_t = jax.ShapeDtypeStruct((chunk * heads, hd), BF16)
    return pl.pallas_call(
        functools.partial(qkv_kernel, heads, hd, group),
        grid_spec=pltpu.PrefetchScalarGridSpec(
            num_scalar_prefetch=1,
            grid=(heads // group,),
            in_specs=[hbm] * 4 + [pl.BlockSpec((feats, wide), lambda n, s: (0, n)), pl.BlockSpec(b.shape, lambda n, s: (0,))],
            out_specs=[out_h, out_h, out_h, out_i, out_i],
            scratch_shapes=[pltpu.VMEM((chunk, feats), BF16)] + [pltpu.VMEM((chunk * heads, hd), F32)] * 2 + [pltpu.SemaphoreType.DMA((4,))],
        ),
        out_shape=[h_t, h_t, h_t, i_t, i_t],
        compiler_params=pltpu.CompilerParams(vmem_limit_bytes=VMEM_BIG),
        cost_estimate=pl.CostEstimate(flops=2 * chunk * feats * w.shape[1], bytes_accessed=w.size * 2 + chunk * feats * 2, transcendentals=0),
        name="qkv",
    )(idx, *pieces, w, b)


def attn_kernel(seq, heads, idx_ref, len_ref, slope_ref, q_ref, kn_ref, vn_ref, kt_ref, vt_ref, ki_ref, vi_ref,
                ko_in, vo_in, c0, c1, c2, c3, ko_ref, vo_ref, m_s, l_s, acc_s, stage, sems):
    head = pl.program_id(0)
    length = len_ref[seq]
    chunk, hd = q_ref.shape[1], q_ref.shape[2]

    def rows_in(n):
        return pltpu.make_async_copy((ki_ref, vi_ref)[n], stage.at[n], sems.at[n])

    def rows_out(n):
        return pltpu.make_async_copy(stage.at[n], (ko_ref, vo_ref)[n].at[seq, pl.ds(length, chunk)], sems.at[n])

    @pl.when(head == 0)
    def _():
        for n in range(2):
            rows_in(n).start()

    @pl.when(head == 1)
    def _():
        for n in range(2):
            rows_in(n).wait()
            rows_out(n).start()

    scale = LOG2E * hd ** -0.5
    slope = slope_ref[head] * LOG2E
    n_full = length // KB
    rest = length - n_full * KB
    tok = chunk // 4
    halves = range(chunk // QB)

    def scores(qi, k, base):
        q = q_ref[0, qi * QB:(qi + 1) * QB, :]
        s = lax.dot_general(q, k, (((1,), (1,)), ((), ())), preferred_element_type=F32) * scale
        pos = (lax.broadcasted_iota(jnp.int32, (1, KB), 1) + (base - qi * QB)).astype(F32) * slope
        return s + pos

    def lanes_sum(p):
        tot = p[:, :128]
        for n in range(1, KB // 128):
            tot = tot + p[:, n * 128:(n + 1) * 128]
        return tot

    def update(qi, s, v):
        m_prev = m_s[qi]
        m_new = jnp.maximum(m_prev, jnp.max(s, axis=1, keepdims=True))
        alpha = jnp.exp2(m_prev - m_new)
        p = jnp.exp2(s - jnp.tile(m_new, (1, KB // 128)))
        l_s[qi] = l_s[qi] * alpha + lanes_sum(p)
        acc_s[qi] = acc_s[qi] * alpha + jnp.dot(p.astype(BF16), v, preferred_element_type=F32)
        m_s[qi] = m_new

    for qi in halves:
        new = slice(qi * QB, (qi + 1) * QB)
        s = scores(qi, kn_ref[0, new, :], qi * QB)
        row = lax.broadcasted_iota(jnp.int32, (QB, KB), 0)
        col = lax.broadcasted_iota(jnp.int32, (QB, KB), 1)
        s = jnp.where(col <= row, s, MASKED)
        m_new = jnp.broadcast_to(jnp.max(s, axis=1, keepdims=True), (QB, 128))
        p = jnp.exp2(s - jnp.tile(m_new, (1, KB // 128)))
        m_s[qi] = m_new
        l_s[qi] = lanes_sum(p)
        acc_s[qi] = jnp.dot(p.astype(BF16), vn_ref[0, new, :], preferred_element_type=F32)

    for qi in halves:
        for kj in range(qi):
            blk = slice(kj * KB, (kj + 1) * KB)
            update(qi, scores(qi, kn_ref[0, blk, :], kj * KB), vn_ref[0, blk, :])

    def old_block(n, carry):
        start = pl.multiple_of(n * KB, KB)
        k, v = kt_ref[0, 0, pl.ds(start, KB), :], vt_ref[0, 0, pl.ds(start, KB), :]
        s = [scores(qi, k, start - length) for qi in halves]
        for qi in halves:
            update(qi, s[qi], v)
        return carry

    lax.fori_loop(0, n_full, old_block, 0)

    @pl.when(rest > 0)
    def _():
        start = pl.multiple_of(n_full * KB, KB)
        k, v = kt_ref[0, 0, pl.ds(start, KB), :], vt_ref[0, 0, pl.ds(start, KB), :]
        inside = lax.broadcasted_iota(jnp.int32, (QB, KB), 1) < rest
        for qi in halves:
            update(qi, jnp.where(inside, scores(qi, k, start - length), MASKED), v)

    for qi in halves:
        ctx = (acc_s[qi] / jnp.sum(l_s[qi], axis=1, keepdims=True)).astype(BF16)
        for j in range(QB // tok):
            owner = idx_ref[0] ^ (qi * (QB // tok) + j)
            for n, out in enumerate((c0, c1, c2, c3)):
                @pl.when(owner == n)
                def _(out=out, j=j, ctx=ctx):
                    out[...] = ctx[j * tok:(j + 1) * tok, :]

    @pl.when(head == heads - 1)
    def _():
        for n in range(2):
            rows_out(n).wait()


def attend(seq, idx, lens, slopes, q, kn, vn, kt, vt, ki, vi, ko, vo):
    heads, chunk, hd = q.shape
    toks = kt.shape[2]
    tok = chunk // 4
    per_head = pl.BlockSpec((1, chunk, hd), lambda h, *_: (h, 0, 0))
    old = pl.BlockSpec((1, 1, toks, hd), lambda h, *_: (seq, h, 0, 0))
    hbm = pl.BlockSpec(memory_space=pl.ANY)
    piece = pl.BlockSpec((tok, hd), lambda h, *_: (0, h))
    piece_t = jax.ShapeDtypeStruct((tok, heads * hd), BF16)
    cache_t = jax.ShapeDtypeStruct(ko.shape, BF16)
    pairs = heads * chunk * (toks // 2 + chunk // 2)
    return pl.pallas_call(
        functools.partial(attn_kernel, seq, heads),
        grid_spec=pltpu.PrefetchScalarGridSpec(
            num_scalar_prefetch=3,
            grid=(heads,),
            in_specs=[per_head] * 3 + [old, old, hbm, hbm, hbm, hbm],
            out_specs=[piece] * 4 + [hbm, hbm],
            scratch_shapes=[pltpu.VMEM((chunk // QB, QB, 128), F32), pltpu.VMEM((chunk // QB, QB, 128), F32), pltpu.VMEM((chunk // QB, QB, hd), F32), pltpu.VMEM((2, *ki.shape), BF16),
                            pltpu.SemaphoreType.DMA((2,))],
        ),
        out_shape=[piece_t] * 4 + [cache_t, cache_t],
        input_output_aliases={10: 4, 11: 5},
        compiler_params=pltpu.CompilerParams(vmem_limit_bytes=VMEM_BIG, has_side_effects=True),
        cost_estimate=pl.CostEstimate(flops=8 * pairs * hd, bytes_accessed=4 * heads * toks * hd, transcendentals=pairs),
        name="attend",
    )(idx, lens, slopes, q, kn, vn, kt, vt, ki, vi, ko, vo)


def out_kernel(seqs, far_row, *refs):
    refs = list(refs)
    take = lambda n: [refs.pop(0) for _ in range(n)]
    (idx_ref,) = take(1)
    xs, ctx = take(1)[0], [take(4) for _ in seqs]
    near, far = take(2), [take(4), take(4)]
    b_ref, g_ref, lb_ref, r_ref, n_ref, xb, cb, wb, acc, xsem, csem, wsem = refs
    tok = ctx[0][0].shape[0]
    part = near[0].shape[0]
    few = part // 4
    copies = [pltpu.make_async_copy(xs.at[pl.ds(seqs[0], len(seqs))], xb, xsem)]
    for i in range(len(seqs)):
        for k in range(4):
            copies.append(pltpu.make_async_copy(ctx[i][k], cb.at[i * tok:(i + 1) * tok, k * part:(k + 1) * part], csem.at[i, k]))
    first_w = len(copies)
    parts = [[pltpu.make_async_copy(near[a], wb.at[a * part:(a + 1) * part], wsem.at[a, 0])] for a in range(2)]
    for a in range(2):
        parts.append([])
        for n in range(4):
            at = pl.ds(pl.multiple_of((a + 2) * part + (idx_ref[1] ^ n) * few, few), few)
            parts[-1].append(pltpu.make_async_copy(far[a][n].at[far_row:far_row + few], wb.at[at], wsem.at[a + 2, n]))
    copies += [c for group in parts for c in group]
    for copy in copies:
        copy.start()
    for copy in copies[:first_w]:
        copy.wait()
    for k in range(4):
        for copy in parts[k]:
            copy.wait()
        total = jnp.dot(cb[:, k * part:(k + 1) * part], wb[k * part:(k + 1) * part, :], preferred_element_type=F32)
        acc[...] = total if k == 0 else acc[...] + total
    for i in range(len(seqs)):
        rows = slice(i * tok, (i + 1) * tok)
        res = (xb[i].astype(F32) + acc[rows, :] + row_of(b_ref)).astype(BF16)
        r_ref[rows, :] = res
        n_ref[rows, :] = ln_rows(res, row_of(g_ref), row_of(lb_ref))


def out_proj(idx, x, seqs, ctx, near, far, far_row, b, g, lb):
    tok, feats = x.shape[1:]
    rows = tok * len(seqs)
    flat = [c for got in ctx for c in got]
    vec = pl.BlockSpec(b.shape, lambda n, s: (0,))
    hbm = pl.BlockSpec(memory_space=pl.ANY)
    t = jax.ShapeDtypeStruct((rows, feats), BF16)
    out = pl.BlockSpec((rows, feats), lambda n, s: (0, 0))
    return pl.pallas_call(
        functools.partial(out_kernel, seqs, far_row),
        grid_spec=pltpu.PrefetchScalarGridSpec(
            num_scalar_prefetch=1, grid=(1,),
            in_specs=[hbm] * (1 + len(flat) + 10) + [vec] * 3, out_specs=[out, out],
            scratch_shapes=[pltpu.VMEM((len(seqs), tok, feats), BF16), pltpu.VMEM((rows, feats), BF16), pltpu.VMEM((feats, feats), BF16),
                            pltpu.VMEM((rows, feats), F32), pltpu.SemaphoreType.DMA, pltpu.SemaphoreType.DMA((len(seqs), 4)), pltpu.SemaphoreType.DMA((4, 4))],
        ),
        out_shape=[t, t],
        compiler_params=pltpu.CompilerParams(vmem_limit_bytes=VMEM_BIG),
        cost_estimate=pl.CostEstimate(flops=2 * rows * feats * feats, bytes_accessed=2 * feats * feats, transcendentals=0),
        name="outp",
    )(idx, x, *flat, *near, *far[0], *far[1], b, g, lb)


def mlp_kernel(near, groups, bias_row, *refs):
    refs = list(refs)
    take = lambda n: [refs.pop(0) for _ in range(n)]
    norms = take(groups)
    bias_refs = take(2) if near else None
    n_arr = 2 if near else 8
    ups, downs = take(n_arr), take(n_arr)
    acc_in, res, bd_ref = (None, None, None) if near else (take(groups), take(groups), take(1)[0])
    (out,) = take(1)
    nb, rb, acc, ubuf, dbuf, bbuf, nsem, rsem, asem, usem, dsem, bsem = refs
    step = pl.program_id(0)
    n_steps = 4
    feats, width = ubuf.shape[2:]
    half = acc.shape[0] if acc.shape[0] <= MLP_ROWS else acc.shape[0] // 2

    def piece_copies(i, a):
        slot = i % 2
        if near:
            cols = slice(i * width, (i + 1) * width)
            up, down = ups[a].at[:, cols], downs[a].at[cols, :]
        else:
            up, down = ups[4 * a + i].at[:feats], downs[4 * a + i].at[:width]
        copies = [pltpu.make_async_copy(down, dbuf.at[slot, a * width:(a + 1) * width], dsem.at[slot, a]),
                  pltpu.make_async_copy(up, ubuf.at[slot, a], usem.at[slot, a])]
        if not near:
            copies.append(pltpu.make_async_copy(ups[4 * a + i].at[bias_row:bias_row + 16], bbuf.at[slot, a], bsem.at[slot, a]))
        return copies

    def rows_of(arrays, dst, sem):
        at, copies = 0, []
        for n, a in enumerate(arrays):
            copies.append(pltpu.make_async_copy(a, dst.at[at:at + a.shape[0]], sem.at[n]))
            at += a.shape[0]
        return copies

    def await_at(i, which):
        @pl.when(step == i)
        def _():
            for copy in which(i):
                copy.wait()

    @pl.when(step == 0)
    def _():
        for copy in rows_of(norms, nb, nsem) + [c for a in range(2) for c in piece_copies(0, a)]:
            copy.start()
        if near:
            acc[...] = jnp.zeros_like(acc)
        else:
            for copy in rows_of(acc_in, acc, asem) + rows_of(res, rb, rsem):
                copy.start()
        for copy in rows_of(norms, nb, nsem):
            copy.wait()

    for i in range(1, n_steps):
        @pl.when(step + 1 == i)
        def _(i=i):
            for copy in [c for a in range(2) for c in piece_copies(i, a)]:
                copy.start()

    slot = lax.rem(step, 2)
    for n in range(acc.shape[0] // half):
        rows = slice(n * half, (n + 1) * half)
        acts = []
        for a in range(2):
            if n == 0:
                for i in range(n_steps):
                    await_at(i, lambda i, a=a: piece_copies(i, a)[1:])
            bias = row_of(bias_refs[a], pl.ds(pl.multiple_of(step * width, width), width)) if near else bbuf[slot, a][:1, :].astype(F32)
            pre = jnp.dot(nb[rows, :], ubuf[slot, a], preferred_element_type=F32) + bias
            acts.append(jax.nn.gelu(pre, approximate=True).astype(BF16))
        if n == 0:
            for i in range(n_steps):
                await_at(i, lambda i: piece_copies(i, 0)[:1] + piece_copies(i, 1)[:1])
            if not near:
                await_at(0, lambda i: rows_of(acc_in, acc, asem))
        acc[rows, :] += jnp.dot(jnp.concatenate(acts, axis=1), dbuf[slot], preferred_element_type=F32)

    @pl.when(step == n_steps - 1)
    def _():
        if near:
            copy = pltpu.make_async_copy(acc, out, asem.at[0])
            copy.start()
            copy.wait()
        else:
            for copy in rows_of(res, rb, rsem):
                copy.wait()
            tok = out.shape[1]
            for n in range(out.shape[0]):
                rows = slice(n * tok, (n + 1) * tok)
                out[n] = (rb[rows, :].astype(F32) + acc[rows, :] + row_of(bd_ref)).astype(BF16)


def mlp(norms, bias, ups, downs, width, seqs, acc=None, res=None, bd=None, bias_row=None):
    feats = norms[0].shape[1]
    rows = sum(a.shape[0] for a in norms)
    whole = lambda a: pl.BlockSpec(a.shape, lambda n: (0,) * len(a.shape))
    hbm = pl.BlockSpec(memory_space=pl.ANY)
    near = acc is None
    if near:
        args = [*norms, *bias, *ups, *downs]
        specs = [hbm] * len(norms) + [whole(v) for v in bias] + [hbm] * (2 * len(ups))
        out_t, out_spec = jax.ShapeDtypeStruct((rows, feats), F32), hbm
    else:
        args = [*norms, *ups, *downs, *acc, *res, bd]
        specs = [hbm] * (len(args) - 1) + [whole(bd)]
        out_t = jax.ShapeDtypeStruct((seqs, rows // seqs, feats), BF16)
        out_spec = whole(out_t)
    return pl.pallas_call(
        functools.partial(mlp_kernel, near, len(norms), bias_row),
        grid=(4,),
        in_specs=specs, out_specs=out_spec, out_shape=out_t,
        scratch_shapes=[pltpu.VMEM((rows, feats), BF16), pltpu.VMEM((16 if near else rows, feats), BF16), pltpu.VMEM((rows, feats), F32), pltpu.VMEM((2, 2, feats, width), BF16),
                        pltpu.VMEM((2, 2 * width, feats), BF16), pltpu.VMEM((2, 2, 16, width), BF16), pltpu.SemaphoreType.DMA((len(norms),)), pltpu.SemaphoreType.DMA((len(norms),)),
                        pltpu.SemaphoreType.DMA((len(norms),)), pltpu.SemaphoreType.DMA((2, 2)), pltpu.SemaphoreType.DMA((2, 2)), pltpu.SemaphoreType.DMA((2, 2))],
        compiler_params=pltpu.CompilerParams(vmem_limit_bytes=VMEM_BIG),
        cost_estimate=pl.CostEstimate(flops=4 * rows * feats * 8 * width, bytes_accessed=4 * feats * 8 * width, transcendentals=0),
        name="mlp",
    )(*args)


def solution(mesh):
    tp_size, dp_size = mesh.shape['tp'], mesh.shape['dp']
    assert tp_size == 4 and dp_size == 4

    def tp_swap(a, k):
        return lax.ppermute(a, 'tp', [(i, i ^ k) for i in range(tp_size)])

    def dp_swap(a, k):
        return lax.ppermute(a, 'dp', [(i, i ^ k) for i in range(dp_size)])

    def local_layer(x_local, prefix_len, k_cache, v_cache, ln1_gain, ln1_bias, w_qkv, b_qkv, w_out, b_out, ln2_gain, ln2_bias, w_up, b_up, w_down, b_down):
        seqs, tok, feats = x_local.shape
        cache_len, heads, hd = k_cache.shape[1:]
        tp, dp = lax.axis_index('tp'), lax.axis_index('dp')
        idx = jnp.stack([tp, dp]).astype(jnp.int32)
        head_ids = tp * heads + jnp.arange(heads)
        slopes = jnp.exp2(-8.0 * (head_ids + 1).astype(F32) / (heads * tp_size))
        near_bias = [b_up, tp_swap(b_up, 1)]
        wo_s = tp_swap(w_out, 1)
        *normed, up_q, down_q = ln1(x_local, ln1_gain, ln1_bias, b_up, w_up, w_down, w_out, dp_size)
        x_x = [tp_swap(normed[b], 2) for b in range(seqs)]
        x_s = [tp_swap(normed[b], 1) for b in range(seqs)]
        x_xs = [tp_swap(x_x[b], 1) for b in range(seqs)]

        width = w_up.shape[1] // dp_size

        def spread(piece, a, b):
            first = tp_swap(piece, 2)
            one = dp_swap(first, a)
            two = dp_swap(first, b)
            both = dp_swap(one, b)
            got = [first, one, two, both] if a == 1 else [first, two, one, both]
            return got, [tp_swap(a, 1) for a in got]

        up_x, up_xs = spread(up_q, 1, 2)
        down_x, down_xs = spread(down_q, 2, 1)
        up_s, down_s = tp_swap(w_up, 1), tp_swap(w_down, 1)

        flat = (seqs, cache_len * heads, hd)
        ko, vo, kt, vt = prep(prefix_len, k_cache.reshape(flat), v_cache.reshape(flat), heads)
        ko, vo = ko.reshape(k_cache.shape), vo.reshape(v_cache.shape)
        got = []
        inter = (tok * tp_size, heads, hd)
        for b in range(seqs):
            q, kn, vn, ki, vi = qkv(idx, [normed[b], x_s[b], x_x[b], x_xs[b]], w_qkv, b_qkv, heads, hd)
            *ctx, ko, vo = attend(b, idx, prefix_len, slopes, q, kn, vn, kt, vt, ki.reshape(inter), vi.reshape(inter), ko, vo)
            got.append([ctx[0]] + [tp_swap(ctx[k], k) for k in (1, 2, 3)])
        norms, resid, acc = [], [], []
        for some in (tuple(range(seqs - 1)), (seqs - 1,)):
            r, n2 = out_proj(idx, x_local, some, [got[b] for b in some], [w_out, wo_s], [down_x, down_xs], width, b_out, ln2_gain, ln2_bias)
            resid.append(r)
            norms.append(n2)
            acc.append(mlp([n2], near_bias, [w_up, up_s], [w_down, down_s], width, seqs))
        out = mlp(norms, None, up_x + up_xs, down_x + down_xs, width, seqs, acc, resid, b_down, feats)
        return out, ko, vo

    tok_spec = P('dp', 'tp', None)
    cache_spec = P('dp', None, 'tp', None)
    rep = P()
    in_specs = (tok_spec, P('dp'), cache_spec, cache_spec, rep, rep, P(None, 'tp'), P('tp'), P('tp', None), rep, rep, rep, P(None, 'tp'), P('tp'), P('tp', None), rep)
    return jax.shard_map(local_layer, mesh=mesh, in_specs=in_specs, out_specs=(tok_spec, cache_spec, cache_spec), check_vma=False)
```

```python
import functools

import jax
import jax.numpy as jnp
from jax import lax
from jax.experimental import pallas as pl
from jax.experimental.pallas import tpu as pltpu
from jax.sharding import PartitionSpec as P


LN_EPS = 1e-5
LOG2E = 1.4426950408889634
MASKED = -1e30 * LOG2E
F32 = jnp.float32
BF16 = jnp.bfloat16
QB = 512
KB = 512
PREP_TOK = 1024
MLP_ROWS = 512
QKV_GROUP = 2
VMEM_BIG = 60 * 1024 * 1024


def ln_rows(rows, gain, bias):
    rows = rows.astype(F32)
    mean = jnp.mean(rows, axis=-1, keepdims=True)
    centered = rows - mean
    var = jnp.mean(centered * centered, axis=-1, keepdims=True)
    return (centered * lax.rsqrt(var + LN_EPS) * gain + bias).astype(BF16)


def prep_kernel(heads, len_ref, k_ref, v_ref, ko_ref, vo_ref, kt_ref, vt_ref, ks, vs):
    toks = kt_ref.shape[2]
    ko_ref[...] = k_ref[...]
    vo_ref[...] = v_ref[...]

    @pl.when(pl.program_id(1) * toks < len_ref[pl.program_id(0)])
    def _():
        for src, tr, tmp in ((k_ref, kt_ref, ks), (v_ref, vt_ref, vs)):
            tmp[...] = src[0].astype(F32)
            for h in range(heads):
                tr[0, h] = tmp[pl.ds(h, toks, stride=heads), :].astype(BF16)


def prep(lens, kc, vc, heads):
    seqs, rows, hd = kc.shape
    toks = rows // heads
    flat = pl.BlockSpec((1, PREP_TOK * heads, hd), lambda b, j, s: (b, j, 0))
    last = lambda b, s: jnp.maximum((s[b] + PREP_TOK - 1) // PREP_TOK, 1) - 1
    tr = pl.BlockSpec((1, heads, PREP_TOK, hd), lambda b, j, s: (b, 0, jnp.minimum(j, last(b, s)), 0))
    flat_t = jax.ShapeDtypeStruct(kc.shape, BF16)
    tr_t = jax.ShapeDtypeStruct((seqs, heads, toks, hd), BF16)
    return pl.pallas_call(
        functools.partial(prep_kernel, heads),
        grid_spec=pltpu.PrefetchScalarGridSpec(
            num_scalar_prefetch=1,
            grid=(seqs, toks // PREP_TOK),
            in_specs=[flat, flat],
            out_specs=[flat, flat, tr, tr],
            scratch_shapes=[pltpu.VMEM((PREP_TOK * heads, hd), F32)] * 2,
        ),
        out_shape=[flat_t, flat_t, tr_t, tr_t],
        compiler_params=pltpu.CompilerParams(vmem_limit_bytes=VMEM_BIG),
        cost_estimate=pl.CostEstimate(flops=int(2e10), bytes_accessed=kc.size * 12, transcendentals=0),
        name="prep",
    )(lens, kc, vc)


def row_of(ref, n=None):
    vec = ref[...] if n is None else ref[n]
    return vec.astype(F32).reshape(1, -1)


def ln1_kernel(seqs, idx_ref, x_ref, g_ref, lb_ref, bu_ref, up_ref, down_ref, wo_ref, *refs):
    outs, (upq, downq, woq, buf, ub, db, sems, isems, osems) = refs[:seqs], refs[seqs:]
    seq = pl.program_id(0)
    dp = lax.axis_index("dp")
    feats, width = up_ref.shape[0], ub.shape[1]
    few = db.shape[0] - width
    cols = lambda n: pl.ds(pl.multiple_of(dp * n, n), n)
    ins = [pltpu.make_async_copy(up_ref.at[:, cols(width)], ub.at[:feats], isems.at[0]),
           pltpu.make_async_copy(down_ref.at[cols(width)], db.at[:width], isems.at[1]),
           pltpu.make_async_copy(wo_ref.at[cols(few)], db.at[width:], isems.at[2])]
    packs = [pltpu.make_async_copy(ub, upq, osems.at[0]), pltpu.make_async_copy(db.at[:width], downq, osems.at[1]),
             pltpu.make_async_copy(db.at[width:], woq, osems.at[2])]

    @pl.when(seq == 0)
    def _():
        for copy in ins:
            copy.start()
        ub[feats:, :] = jnp.broadcast_to(row_of(bu_ref, cols(width)), (ub.shape[0] - feats, width)).astype(BF16)

    normed = ln_rows(x_ref[0], row_of(g_ref), row_of(lb_ref))
    for n in range(seqs):
        @pl.when(seq == n)
        def _(n=n):
            buf[n] = normed
            pltpu.make_async_copy(buf.at[n], outs[n], sems.at[n]).start()

    @pl.when(seq == seqs - 1)
    def _():
        for copy in ins:
            copy.wait()
        for copy in packs:
            copy.start()
        for n in range(seqs):
            pltpu.make_async_copy(buf.at[n], outs[n], sems.at[n]).wait()
        for copy in packs:
            copy.wait()


def ln1(idx, x, g, b, bu, w_up, w_down, w_out, parts):
    seqs, tok, feats = x.shape
    up_t = jax.ShapeDtypeStruct((feats + 16, w_up.shape[1] // parts), BF16)
    down_t = jax.ShapeDtypeStruct((w_down.shape[0] // parts, feats), BF16)
    wo_t = jax.ShapeDtypeStruct((w_out.shape[0] // parts, feats), BF16)
    hbm = pl.BlockSpec(memory_space=pl.ANY)
    return pl.pallas_call(
        functools.partial(ln1_kernel, seqs),
        grid_spec=pltpu.PrefetchScalarGridSpec(
            num_scalar_prefetch=1,
            grid=(seqs,),
            in_specs=[pl.BlockSpec((1, tok, feats), lambda n, s: (s[2 + n], 0, 0)), *[pl.BlockSpec(v.shape, lambda n, s: (0,)) for v in (g, b, bu)], hbm, hbm, hbm],
            out_specs=[hbm] * (seqs + 3),
            scratch_shapes=[pltpu.VMEM((seqs, tok, feats), BF16), pltpu.VMEM(up_t.shape, BF16), pltpu.VMEM((down_t.shape[0] + wo_t.shape[0], feats), BF16),
                            pltpu.SemaphoreType.DMA((seqs,)), pltpu.SemaphoreType.DMA((3,)), pltpu.SemaphoreType.DMA((3,))],
        ),
        out_shape=[jax.ShapeDtypeStruct((tok, feats), BF16)] * seqs + [up_t, down_t, wo_t],
        compiler_params=pltpu.CompilerParams(vmem_limit_bytes=VMEM_BIG),
        cost_estimate=pl.CostEstimate(flops=int(2e9), bytes_accessed=x.size * 8, transcendentals=0),
        name="ln1",
    )(idx, x, g, b, bu, w_up, w_down, w_out)


def qkv_kernel(heads, hd, group, idx_ref, p0, p1, p2, p3, w_ref, b_ref,
               q_ref, k_ref, v_ref, ki_ref, vi_ref, norm_s, ks, vs, sems):
    step = pl.program_id(0)
    chunk = norm_s.shape[0]
    toks = chunk // 4

    @pl.when(step == 0)
    def _():
        copies = []
        for n, piece in enumerate((p0, p1, p2, p3)):
            at = pl.ds(pl.multiple_of((idx_ref[0] ^ n) * toks, toks), toks)
            copies.append(pltpu.make_async_copy(piece, norm_s.at[at], sems.at[n]))
        for copy in copies:
            copy.start()
        for copy in copies:
            copy.wait()

    bias = row_of(b_ref)
    bias = jnp.where(step == 0, bias[:, :w_ref.shape[1]], bias[:, w_ref.shape[1]:])
    out = jnp.dot(norm_s[...], w_ref[...], preferred_element_type=F32) + bias
    for n in range(group):
        c0 = n * 3 * hd
        k = out[:, c0 + hd:c0 + 2 * hd]
        v = out[:, c0 + 2 * hd:c0 + 3 * hd]
        q_ref[n] = out[:, c0:c0 + hd].astype(BF16)
        k_ref[n] = k.astype(BF16)
        v_ref[n] = v.astype(BF16)
        ks[pl.ds(step * group + n, chunk, stride=heads), :] = k
        vs[pl.ds(step * group + n, chunk, stride=heads), :] = v

    @pl.when(step == heads // group - 1)
    def _():
        ki_ref[...] = ks[...].astype(BF16)
        vi_ref[...] = vs[...].astype(BF16)


def qkv(idx, pieces, w, b, heads, hd):
    toks, feats = pieces[0].shape
    chunk = toks * len(pieces)
    group = QKV_GROUP
    wide = group * 3 * hd
    hbm = pl.BlockSpec(memory_space=pl.ANY)
    out_h = pl.BlockSpec((group, chunk, hd), lambda n, s: (n, 0, 0))
    out_i = pl.BlockSpec((chunk * heads, hd), lambda n, s: (0, 0))
    h_t = jax.ShapeDtypeStruct((heads, chunk, hd), BF16)
    i_t = jax.ShapeDtypeStruct((chunk * heads, hd), BF16)
    return pl.pallas_call(
        functools.partial(qkv_kernel, heads, hd, group),
        grid_spec=pltpu.PrefetchScalarGridSpec(
            num_scalar_prefetch=1,
            grid=(heads // group,),
            in_specs=[hbm] * 4 + [pl.BlockSpec((feats, wide), lambda n, s: (0, n)), pl.BlockSpec(b.shape, lambda n, s: (0,))],
            out_specs=[out_h, out_h, out_h, out_i, out_i],
            scratch_shapes=[pltpu.VMEM((chunk, feats), BF16)] + [pltpu.VMEM((chunk * heads, hd), F32)] * 2 + [pltpu.SemaphoreType.DMA((4,))],
        ),
        out_shape=[h_t, h_t, h_t, i_t, i_t],
        compiler_params=pltpu.CompilerParams(vmem_limit_bytes=VMEM_BIG),
        cost_estimate=pl.CostEstimate(flops=2 * chunk * feats * w.shape[1], bytes_accessed=w.size * 2 + chunk * feats * 2, transcendentals=0),
        name="qkv",
    )(idx, *pieces, w, b)


def attn_kernel(place, heads, idx_ref, len_ref, slope_ref, q_ref, kn_ref, vn_ref, kt_ref, vt_ref, ki_ref, vi_ref,
                ko_in, vo_in, c0, c1, c2, c3, ko_ref, vo_ref, m_s, l_s, acc_s, stage, sems):
    head = pl.program_id(0)
    seq = idx_ref[2 + place]
    length = len_ref[seq]
    chunk, hd = q_ref.shape[1], q_ref.shape[2]

    def rows_in(n):
        return pltpu.make_async_copy((ki_ref, vi_ref)[n], stage.at[n], sems.at[n])

    def rows_out(n):
        return pltpu.make_async_copy(stage.at[n], (ko_ref, vo_ref)[n].at[seq, pl.ds(length, chunk)], sems.at[n])

    @pl.when(head == 0)
    def _():
        for n in range(2):
            rows_in(n).start()

    @pl.when(head == 1)
    def _():
        for n in range(2):
            rows_in(n).wait()
            rows_out(n).start()

    scale = LOG2E * hd ** -0.5
    slope = slope_ref[head] * LOG2E
    n_full = length // KB
    rest = length - n_full * KB
    tok = chunk // 4
    halves = range(chunk // QB)

    def scores(qi, k, base):
        q = q_ref[0, qi * QB:(qi + 1) * QB, :]
        s = lax.dot_general(q, k, (((1,), (1,)), ((), ())), preferred_element_type=F32) * scale
        pos = (lax.broadcasted_iota(jnp.int32, (1, KB), 1) + (base - qi * QB)).astype(F32) * slope
        return s + pos

    def lanes_sum(p):
        tot = p[:, :128]
        for n in range(1, KB // 128):
            tot = tot + p[:, n * 128:(n + 1) * 128]
        return tot

    def update(qi, s, v):
        m_prev = m_s[qi]
        m_new = jnp.maximum(m_prev, jnp.max(s, axis=1, keepdims=True))
        alpha = jnp.exp2(m_prev - m_new)
        p = jnp.exp2(s - jnp.tile(m_new, (1, KB // 128)))
        l_s[qi] = l_s[qi] * alpha + lanes_sum(p)
        acc_s[qi] = acc_s[qi] * alpha + jnp.dot(p.astype(BF16), v, preferred_element_type=F32)
        m_s[qi] = m_new

    for qi in halves:
        new = slice(qi * QB, (qi + 1) * QB)
        s = scores(qi, kn_ref[0, new, :], qi * QB)
        row = lax.broadcasted_iota(jnp.int32, (QB, KB), 0)
        col = lax.broadcasted_iota(jnp.int32, (QB, KB), 1)
        s = jnp.where(col <= row, s, MASKED)
        m_new = jnp.broadcast_to(jnp.max(s, axis=1, keepdims=True), (QB, 128))
        p = jnp.exp2(s - jnp.tile(m_new, (1, KB // 128)))
        m_s[qi] = m_new
        l_s[qi] = lanes_sum(p)
        acc_s[qi] = jnp.dot(p.astype(BF16), vn_ref[0, new, :], preferred_element_type=F32)

    for qi in halves:
        for kj in range(qi):
            blk = slice(kj * KB, (kj + 1) * KB)
            update(qi, scores(qi, kn_ref[0, blk, :], kj * KB), vn_ref[0, blk, :])

    def old_block(n, carry):
        start = pl.multiple_of(n * KB, KB)
        k, v = kt_ref[0, 0, pl.ds(start, KB), :], vt_ref[0, 0, pl.ds(start, KB), :]
        s = [scores(qi, k, start - length) for qi in halves]
        for qi in halves:
            update(qi, s[qi], v)
        return carry

    lax.fori_loop(0, n_full, old_block, 0)

    @pl.when(rest > 0)
    def _():
        start = pl.multiple_of(n_full * KB, KB)
        k, v = kt_ref[0, 0, pl.ds(start, KB), :], vt_ref[0, 0, pl.ds(start, KB), :]
        inside = lax.broadcasted_iota(jnp.int32, (QB, KB), 1) < rest
        for qi in halves:
            update(qi, jnp.where(inside, scores(qi, k, start - length), MASKED), v)

    for qi in halves:
        ctx = (acc_s[qi] / jnp.sum(l_s[qi], axis=1, keepdims=True)).astype(BF16)
        for j in range(QB // tok):
            owner = idx_ref[0] ^ (qi * (QB // tok) + j)
            for n, out in enumerate((c0, c1, c2, c3)):
                @pl.when(owner == n)
                def _(out=out, j=j, ctx=ctx):
                    out[...] = ctx[j * tok:(j + 1) * tok, :]

    @pl.when(head == heads - 1)
    def _():
        for n in range(2):
            rows_out(n).wait()


def attend(place, idx, lens, slopes, q, kn, vn, kt, vt, ki, vi, ko, vo):
    heads, chunk, hd = q.shape
    toks = kt.shape[2]
    tok = chunk // 4
    per_head = pl.BlockSpec((1, chunk, hd), lambda h, *_: (h, 0, 0))
    old = pl.BlockSpec((1, 1, toks, hd), lambda h, s, *_: (s[2 + place], h, 0, 0))
    hbm = pl.BlockSpec(memory_space=pl.ANY)
    piece = pl.BlockSpec((tok, hd), lambda h, *_: (0, h))
    piece_t = jax.ShapeDtypeStruct((tok, heads * hd), BF16)
    cache_t = jax.ShapeDtypeStruct(ko.shape, BF16)
    pairs = heads * chunk * (toks // 2 + chunk // 2)
    return pl.pallas_call(
        functools.partial(attn_kernel, place, heads),
        grid_spec=pltpu.PrefetchScalarGridSpec(
            num_scalar_prefetch=3,
            grid=(heads,),
            in_specs=[per_head] * 3 + [old, old, hbm, hbm, hbm, hbm],
            out_specs=[piece] * 4 + [hbm, hbm],
            scratch_shapes=[pltpu.VMEM((chunk // QB, QB, 128), F32), pltpu.VMEM((chunk // QB, QB, 128), F32), pltpu.VMEM((chunk // QB, QB, hd), F32), pltpu.VMEM((2, *ki.shape), BF16),
                            pltpu.SemaphoreType.DMA((2,))],
        ),
        out_shape=[piece_t] * 4 + [cache_t, cache_t],
        input_output_aliases={10: 4, 11: 5},
        compiler_params=pltpu.CompilerParams(vmem_limit_bytes=VMEM_BIG, has_side_effects=True),
        cost_estimate=pl.CostEstimate(flops=8 * pairs * hd, bytes_accessed=4 * heads * toks * hd, transcendentals=pairs),
        name="attend",
    )(idx, lens, slopes, q, kn, vn, kt, vt, ki, vi, ko, vo)


def out_kernel(seqs, *refs):
    refs = list(refs)
    take = lambda n: [refs.pop(0) for _ in range(n)]
    (idx_ref,) = take(1)
    xs, ctx = take(1)[0], [take(4) for _ in seqs]
    near, far = take(2), [take(4), take(4)]
    b_ref, g_ref, lb_ref, r_ref, n_ref, xb, cb, wb, acc, xsem, csem, wsem = refs
    tok = ctx[0][0].shape[0]
    part = near[0].shape[0]
    few = part // 4
    copies = [pltpu.make_async_copy(xs.at[idx_ref[2 + n]], xb.at[i], xsem.at[i]) for i, n in enumerate(seqs)]
    for i in range(len(seqs)):
        for k in range(4):
            copies.append(pltpu.make_async_copy(ctx[i][k], cb.at[i * tok:(i + 1) * tok, k * part:(k + 1) * part], csem.at[i, k]))
    first_w = len(copies)
    parts = [[pltpu.make_async_copy(near[a], wb.at[a * part:(a + 1) * part], wsem.at[a, 0])] for a in range(2)]
    for a in range(2):
        parts.append([])
        for n in range(4):
            at = pl.ds(pl.multiple_of((a + 2) * part + (idx_ref[1] ^ n) * few, few), few)
            parts[-1].append(pltpu.make_async_copy(far[a][n], wb.at[at], wsem.at[a + 2, n]))
    copies += [c for group in parts for c in group]
    for copy in copies:
        copy.start()
    for copy in copies[:first_w]:
        copy.wait()
    for k in range(4):
        for copy in parts[k]:
            copy.wait()
        total = jnp.dot(cb[:, k * part:(k + 1) * part], wb[k * part:(k + 1) * part, :], preferred_element_type=F32)
        acc[...] = total if k == 0 else acc[...] + total
    for i in range(len(seqs)):
        rows = slice(i * tok, (i + 1) * tok)
        res = (xb[i].astype(F32) + acc[rows, :] + row_of(b_ref)).astype(BF16)
        r_ref[rows, :] = res
        n_ref[rows, :] = ln_rows(res, row_of(g_ref), row_of(lb_ref))


def out_proj(idx, x, seqs, ctx, near, far, b, g, lb):
    tok, feats = x.shape[1:]
    rows = tok * len(seqs)
    flat = [c for got in ctx for c in got]
    vec = pl.BlockSpec(b.shape, lambda n, s: (0,))
    hbm = pl.BlockSpec(memory_space=pl.ANY)
    t = jax.ShapeDtypeStruct((rows, feats), BF16)
    out = pl.BlockSpec((rows, feats), lambda n, s: (0, 0))
    return pl.pallas_call(
        functools.partial(out_kernel, seqs),
        grid_spec=pltpu.PrefetchScalarGridSpec(
            num_scalar_prefetch=1, grid=(1,),
            in_specs=[hbm] * (1 + len(flat) + 10) + [vec] * 3, out_specs=[out, out],
            scratch_shapes=[pltpu.VMEM((len(seqs), tok, feats), BF16), pltpu.VMEM((rows, feats), BF16), pltpu.VMEM((feats, feats), BF16),
                            pltpu.VMEM((rows, feats), F32), pltpu.SemaphoreType.DMA((len(seqs),)), pltpu.SemaphoreType.DMA((len(seqs), 4)), pltpu.SemaphoreType.DMA((4, 4))],
        ),
        out_shape=[t, t],
        compiler_params=pltpu.CompilerParams(vmem_limit_bytes=VMEM_BIG),
        cost_estimate=pl.CostEstimate(flops=2 * rows * feats * feats, bytes_accessed=2 * feats * feats, transcendentals=0),
        name="outp",
    )(idx, x, *flat, *near, *far[0], *far[1], b, g, lb)


def mlp_kernel(near, groups, bias_row, *refs):
    refs = list(refs)
    take = lambda n: [refs.pop(0) for _ in range(n)]
    (idx_ref,) = take(1)
    norms = take(groups)
    bias_refs = take(2) if near else None
    n_arr = 2 if near else 8
    ups, downs = take(n_arr), take(n_arr)
    acc_in, res, bd_ref = (None, None, None) if near else (take(groups), take(groups), take(1)[0])
    (out,) = take(1)
    nb, rb, acc, ubuf, dbuf, bbuf, nsem, rsem, asem, usem, dsem, bsem = refs
    step = pl.program_id(0)
    n_steps = 4
    feats, width = ubuf.shape[2:]
    half = acc.shape[0] if acc.shape[0] <= MLP_ROWS else acc.shape[0] // 2

    def piece_copies(i, a):
        slot = i % 2
        if near:
            cols = slice(i * width, (i + 1) * width)
            up, down = ups[a].at[:, cols], downs[a].at[cols, :]
        else:
            up, down = ups[4 * a + i].at[:feats], downs[4 * a + i]
        copies = [pltpu.make_async_copy(down, dbuf.at[slot, a * width:(a + 1) * width], dsem.at[slot, a]),
                  pltpu.make_async_copy(up, ubuf.at[slot, a], usem.at[slot, a])]
        if not near:
            copies.append(pltpu.make_async_copy(ups[4 * a + i].at[bias_row:bias_row + 16], bbuf.at[slot, a], bsem.at[slot, a]))
        return copies

    def rows_of(arrays, dst, sem):
        at, copies = 0, []
        for n, a in enumerate(arrays):
            copies.append(pltpu.make_async_copy(a, dst.at[at:at + a.shape[0]], sem.at[n]))
            at += a.shape[0]
        return copies

    def await_at(i, which):
        @pl.when(step == i)
        def _():
            for copy in which(i):
                copy.wait()

    @pl.when(step == 0)
    def _():
        for copy in rows_of(norms, nb, nsem) + [c for a in range(2) for c in piece_copies(0, a)]:
            copy.start()
        if near:
            acc[...] = jnp.zeros_like(acc)
        else:
            for copy in rows_of(acc_in, acc, asem) + rows_of(res, rb, rsem):
                copy.start()
        for copy in rows_of(norms, nb, nsem):
            copy.wait()

    for i in range(1, n_steps):
        @pl.when(step + 1 == i)
        def _(i=i):
            for copy in [c for a in range(2) for c in piece_copies(i, a)]:
                copy.start()

    slot = lax.rem(step, 2)
    for n in range(acc.shape[0] // half):
        rows = slice(n * half, (n + 1) * half)
        acts = []
        for a in range(2):
            if n == 0:
                for i in range(n_steps):
                    await_at(i, lambda i, a=a: piece_copies(i, a)[1:])
            bias = row_of(bias_refs[a], pl.ds(pl.multiple_of(step * width, width), width)) if near else bbuf[slot, a][:1, :].astype(F32)
            pre = jnp.dot(nb[rows, :], ubuf[slot, a], preferred_element_type=F32) + bias
            acts.append(jax.nn.gelu(pre, approximate=True).astype(BF16))
        if n == 0:
            for i in range(n_steps):
                await_at(i, lambda i: piece_copies(i, 0)[:1] + piece_copies(i, 1)[:1])
            if not near:
                await_at(0, lambda i: rows_of(acc_in, acc, asem))
        acc[rows, :] += jnp.dot(jnp.concatenate(acts, axis=1), dbuf[slot], preferred_element_type=F32)

    @pl.when(step == n_steps - 1)
    def _():
        if near:
            copy = pltpu.make_async_copy(acc, out, asem.at[0])
            copy.start()
            copy.wait()
        else:
            for copy in rows_of(res, rb, rsem):
                copy.wait()
            tok = out.shape[1]
            for n in range(out.shape[0]):
                rows = slice(n * tok, (n + 1) * tok)
                out[idx_ref[2 + n]] = (rb[rows, :].astype(F32) + acc[rows, :] + row_of(bd_ref)).astype(BF16)


def mlp(idx, norms, bias, ups, downs, width, seqs, acc=None, res=None, bd=None, bias_row=None):
    feats = norms[0].shape[1]
    rows = sum(a.shape[0] for a in norms)
    whole = lambda a: pl.BlockSpec(a.shape, lambda n, s: (0,) * len(a.shape))
    hbm = pl.BlockSpec(memory_space=pl.ANY)
    near = acc is None
    if near:
        args = [*norms, *bias, *ups, *downs]
        specs = [hbm] * len(norms) + [whole(v) for v in bias] + [hbm] * (2 * len(ups))
        out_t, out_spec = jax.ShapeDtypeStruct((rows, feats), F32), hbm
    else:
        args = [*norms, *ups, *downs, *acc, *res, bd]
        specs = [hbm] * (len(args) - 1) + [whole(bd)]
        out_t = jax.ShapeDtypeStruct((seqs, rows // seqs, feats), BF16)
        out_spec = whole(out_t)
    return pl.pallas_call(
        functools.partial(mlp_kernel, near, len(norms), bias_row),
        grid_spec=pltpu.PrefetchScalarGridSpec(
            num_scalar_prefetch=1, grid=(4,), in_specs=specs, out_specs=out_spec,
            scratch_shapes=[pltpu.VMEM((rows, feats), BF16), pltpu.VMEM((16 if near else rows, feats), BF16), pltpu.VMEM((rows, feats), F32), pltpu.VMEM((2, 2, feats, width), BF16),
                        pltpu.VMEM((2, 2 * width, feats), BF16), pltpu.VMEM((2, 2, 16, width), BF16), pltpu.SemaphoreType.DMA((len(norms),)), pltpu.SemaphoreType.DMA((len(norms),)),
                        pltpu.SemaphoreType.DMA((len(norms),)), pltpu.SemaphoreType.DMA((2, 2)), pltpu.SemaphoreType.DMA((2, 2)), pltpu.SemaphoreType.DMA((2, 2))],
        ),
        out_shape=out_t,
        compiler_params=pltpu.CompilerParams(vmem_limit_bytes=VMEM_BIG),
        cost_estimate=pl.CostEstimate(flops=4 * rows * feats * 8 * width, bytes_accessed=4 * feats * 8 * width, transcendentals=0),
        name="mlp",
    )(idx, *args)


def solution(mesh):
    tp_size, dp_size = mesh.shape['tp'], mesh.shape['dp']
    assert tp_size == 4 and dp_size == 4

    def tp_swap(a, k):
        return lax.ppermute(a, 'tp', [(i, i ^ k) for i in range(tp_size)])

    def dp_swap(a, k):
        return lax.ppermute(a, 'dp', [(i, i ^ k) for i in range(dp_size)])

    def local_layer(x_local, prefix_len, k_cache, v_cache, ln1_gain, ln1_bias, w_qkv, b_qkv, w_out, b_out, ln2_gain, ln2_bias, w_up, b_up, w_down, b_down):
        seqs, tok, feats = x_local.shape
        cache_len, heads, hd = k_cache.shape[1:]
        tp, dp = lax.axis_index('tp'), lax.axis_index('dp')
        before = (prefix_len[None, :] > prefix_len[:, None]) | ((prefix_len[None, :] == prefix_len[:, None]) & (jnp.arange(seqs)[None, :] < jnp.arange(seqs)[:, None]))
        rank = jnp.sum(before.astype(jnp.int32), axis=1)
        falling = jnp.sum(jnp.where(rank[None, :] == jnp.arange(seqs)[:, None], jnp.arange(seqs)[None, :], 0), axis=1)
        idx = jnp.concatenate([jnp.stack([tp, dp]), falling]).astype(jnp.int32)
        head_ids = tp * heads + jnp.arange(heads)
        slopes = jnp.exp2(-8.0 * (head_ids + 1).astype(F32) / (heads * tp_size))
        near_bias = [b_up, tp_swap(b_up, 1)]
        wo_s = tp_swap(w_out, 1)
        *normed, up_q, down_q, wo_q = ln1(idx, x_local, ln1_gain, ln1_bias, b_up, w_up, w_down, w_out, dp_size)
        x_x = [tp_swap(normed[b], 2) for b in range(seqs)]
        x_s = [tp_swap(normed[b], 1) for b in range(seqs)]
        x_xs = [tp_swap(x_x[b], 1) for b in range(seqs)]

        width = w_up.shape[1] // dp_size

        def spread(piece, a, b):
            first = tp_swap(piece, 2)
            one = dp_swap(first, a)
            two = dp_swap(first, b)
            both = dp_swap(one, b)
            got = [first, one, two, both] if a == 1 else [first, two, one, both]
            return got, [tp_swap(a, 1) for a in got]

        up_x, up_xs = spread(up_q, 1, 2)
        down_x, down_xs = spread(down_q, 2, 1)
        wo_x, wo_xs = spread(wo_q, 1, 2)
        up_s, down_s = tp_swap(w_up, 1), tp_swap(w_down, 1)

        flat = (seqs, cache_len * heads, hd)
        ko, vo, kt, vt = prep(prefix_len, k_cache.reshape(flat), v_cache.reshape(flat), heads)
        ko, vo = ko.reshape(k_cache.shape), vo.reshape(v_cache.shape)
        got = []
        inter = (tok * tp_size, heads, hd)
        for b in range(seqs):
            q, kn, vn, ki, vi = qkv(idx, [normed[b], x_s[b], x_x[b], x_xs[b]], w_qkv, b_qkv, heads, hd)
            *ctx, ko, vo = attend(b, idx, prefix_len, slopes, q, kn, vn, kt, vt, ki.reshape(inter), vi.reshape(inter), ko, vo)
            got.append([ctx[0]] + [tp_swap(ctx[k], k) for k in (1, 2, 3)])
        norms, resid, acc = [], [], []
        for some in (tuple(range(seqs)),):
            r, n2 = out_proj(idx, x_local, some, [got[b] for b in some], [w_out, wo_s], [wo_x, wo_xs], b_out, ln2_gain, ln2_bias)
            resid.append(r)
            norms.append(n2)
            acc.append(mlp(idx, [n2], near_bias, [w_up, up_s], [w_down, down_s], width, seqs))
        out = mlp(idx, norms, None, up_x + up_xs, down_x + down_xs, width, seqs, acc, resid, b_down, feats)
        return out, ko, vo

    tok_spec = P('dp', 'tp', None)
    cache_spec = P('dp', None, 'tp', None)
    rep = P()
    in_specs = (tok_spec, P('dp'), cache_spec, cache_spec, rep, rep, P(None, 'tp'), P('tp'), P('tp', None), rep, rep, rep, P(None, 'tp'), P('tp'), P('tp', None), rep)
    return jax.shard_map(local_layer, mesh=mesh, in_specs=in_specs, out_specs=(tok_spec, cache_spec, cache_spec), check_vma=False)
```

```python
import functools

import jax
import jax.numpy as jnp
from jax import lax
from jax.experimental import pallas as pl
from jax.experimental.pallas import tpu as pltpu
from jax.sharding import PartitionSpec as P


LN_EPS = 1e-5
LOG2E = 1.4426950408889634
MASKED = -1e30 * LOG2E
F32 = jnp.float32
BF16 = jnp.bfloat16
QB = 512
KB = 512
PREP_TOK = 1024
MLP_ROWS = 512
QKV_GROUP = 2
VMEM_BIG = 60 * 1024 * 1024


def ln_rows(rows, gain, bias):
    rows = rows.astype(F32)
    mean = jnp.mean(rows, axis=-1, keepdims=True)
    centered = rows - mean
    var = jnp.mean(centered * centered, axis=-1, keepdims=True)
    return (centered * lax.rsqrt(var + LN_EPS) * gain + bias).astype(BF16)


def prep_kernel(heads, len_ref, k_ref, v_ref, kt_ref, vt_ref, ks, vs):
    toks = kt_ref.shape[2]

    @pl.when((pl.program_id(1) * toks < len_ref[pl.program_id(0)]) | (pl.program_id(1) == 0))
    def _():
        for src, tr, tmp in ((k_ref, kt_ref, ks), (v_ref, vt_ref, vs)):
            tmp[...] = src[0].astype(F32)
            for h in range(heads):
                tr[0, h] = tmp[pl.ds(h, toks, stride=heads), :].astype(BF16)


def prep(lens, kc, vc, heads):
    seqs, rows, hd = kc.shape
    toks = rows // heads
    block = lambda b, j, s: jnp.minimum(j, jnp.maximum((s[b] + PREP_TOK - 1) // PREP_TOK, 1) - 1)
    flat = pl.BlockSpec((1, PREP_TOK * heads, hd), lambda b, j, s: (b, block(b, j, s), 0))
    tr = pl.BlockSpec((1, heads, PREP_TOK, hd), lambda b, j, s: (b, 0, block(b, j, s), 0))
    tr_t = jax.ShapeDtypeStruct((seqs, heads, toks, hd), BF16)
    return pl.pallas_call(
        functools.partial(prep_kernel, heads),
        grid_spec=pltpu.PrefetchScalarGridSpec(
            num_scalar_prefetch=1,
            grid=(seqs, toks // PREP_TOK),
            in_specs=[flat, flat],
            out_specs=[tr, tr],
            scratch_shapes=[pltpu.VMEM((PREP_TOK * heads, hd), F32)] * 2,
        ),
        out_shape=[tr_t, tr_t],
        compiler_params=pltpu.CompilerParams(vmem_limit_bytes=VMEM_BIG),
        cost_estimate=pl.CostEstimate(flops=int(2e10), bytes_accessed=kc.size * 8, transcendentals=0),
        name="prep",
    )(lens, kc, vc)


def row_of(ref, n=None):
    vec = ref[...] if n is None else ref[n]
    return vec.astype(F32).reshape(1, -1)


def ln1_kernel(seqs, idx_ref, x_ref, g_ref, lb_ref, bu_ref, up_ref, down_ref, wo_ref, *refs):
    outs, (upq, uqq, downq, woq, buf, ub, db, sems, isems, osems) = refs[:seqs], refs[seqs:]
    seq = pl.program_id(0)
    dp = lax.axis_index("dp")
    feats, width = up_ref.shape[0], ub.shape[1]
    few = db.shape[0] - width
    cols = lambda n: pl.ds(pl.multiple_of(dp * n, n), n)
    ins = [pltpu.make_async_copy(up_ref.at[:, cols(width)], ub.at[:feats], isems.at[0]),
           pltpu.make_async_copy(down_ref.at[cols(width)], db.at[:width], isems.at[1]),
           pltpu.make_async_copy(wo_ref.at[cols(few)], db.at[width:], isems.at[2])]
    half = width // 2
    packs = [pltpu.make_async_copy(ub.at[:, :half], upq, osems.at[0]), pltpu.make_async_copy(ub.at[:, half:], uqq, osems.at[3]),
             pltpu.make_async_copy(db.at[:width], downq, osems.at[1]),
             pltpu.make_async_copy(db.at[width:], woq, osems.at[2])]

    @pl.when(seq == 0)
    def _():
        for copy in ins:
            copy.start()
        ub[feats:, :] = jnp.broadcast_to(row_of(bu_ref, cols(width)), (ub.shape[0] - feats, width)).astype(BF16)

    normed = ln_rows(x_ref[0], row_of(g_ref), row_of(lb_ref))
    for n in range(seqs):
        @pl.when(seq == n)
        def _(n=n):
            buf[n] = normed
            pltpu.make_async_copy(buf.at[n], outs[n], sems.at[n]).start()

    @pl.when(seq == seqs - 1)
    def _():
        for copy in ins:
            copy.wait()
        for copy in packs:
            copy.start()
        for n in range(seqs):
            pltpu.make_async_copy(buf.at[n], outs[n], sems.at[n]).wait()
        for copy in packs:
            copy.wait()


def ln1(idx, x, g, b, bu, w_up, w_down, w_out, parts):
    seqs, tok, feats = x.shape
    up_t = jax.ShapeDtypeStruct((feats + 16, w_up.shape[1] // parts // 2), BF16)
    down_t = jax.ShapeDtypeStruct((w_down.shape[0] // parts, feats), BF16)
    wo_t = jax.ShapeDtypeStruct((w_out.shape[0] // parts, feats), BF16)
    hbm = pl.BlockSpec(memory_space=pl.ANY)
    return pl.pallas_call(
        functools.partial(ln1_kernel, seqs),
        grid_spec=pltpu.PrefetchScalarGridSpec(
            num_scalar_prefetch=1,
            grid=(seqs,),
            in_specs=[pl.BlockSpec((1, tok, feats), lambda n, s: (s[2 + n], 0, 0)), *[pl.BlockSpec(v.shape, lambda n, s: (0,)) for v in (g, b, bu)], hbm, hbm, hbm],
            out_specs=[hbm] * (seqs + 4),
            scratch_shapes=[pltpu.VMEM((seqs, tok, feats), BF16), pltpu.VMEM((up_t.shape[0], 2 * up_t.shape[1]), BF16), pltpu.VMEM((down_t.shape[0] + wo_t.shape[0], feats), BF16),
                            pltpu.SemaphoreType.DMA((seqs,)), pltpu.SemaphoreType.DMA((3,)), pltpu.SemaphoreType.DMA((4,))],
        ),
        out_shape=[jax.ShapeDtypeStruct((tok, feats), BF16)] * seqs + [up_t, up_t, down_t, wo_t],
        compiler_params=pltpu.CompilerParams(vmem_limit_bytes=VMEM_BIG),
        cost_estimate=pl.CostEstimate(flops=int(2e9), bytes_accessed=x.size * 8, transcendentals=0),
        name="ln1",
    )(idx, x, g, b, bu, w_up, w_down, w_out)


def qkv_kernel(heads, hd, group, idx_ref, p0, p1, p2, p3, w_ref, b_ref,
               q_ref, k_ref, v_ref, ki_ref, vi_ref, norm_s, ks, vs, sems):
    step = pl.program_id(0)
    chunk = norm_s.shape[0]
    toks = chunk // 4

    @pl.when(step == 0)
    def _():
        copies = []
        for n, piece in enumerate((p0, p1, p2, p3)):
            at = pl.ds(pl.multiple_of((idx_ref[0] ^ n) * toks, toks), toks)
            copies.append(pltpu.make_async_copy(piece, norm_s.at[at], sems.at[n]))
        for copy in copies:
            copy.start()
        for copy in copies:
            copy.wait()

    bias = row_of(b_ref)
    bias = jnp.where(step == 0, bias[:, :w_ref.shape[1]], bias[:, w_ref.shape[1]:])
    out = jnp.dot(norm_s[...], w_ref[...], preferred_element_type=F32) + bias
    for n in range(group):
        c0 = n * 3 * hd
        k = out[:, c0 + hd:c0 + 2 * hd]
        v = out[:, c0 + 2 * hd:c0 + 3 * hd]
        q_ref[n] = out[:, c0:c0 + hd].astype(BF16)
        k_ref[n] = k.astype(BF16)
        v_ref[n] = v.astype(BF16)
        ks[pl.ds(step * group + n, chunk, stride=heads), :] = k
        vs[pl.ds(step * group + n, chunk, stride=heads), :] = v

    @pl.when(step == heads // group - 1)
    def _():
        ki_ref[...] = ks[...].astype(BF16)
        vi_ref[...] = vs[...].astype(BF16)


def qkv(idx, pieces, w, b, heads, hd):
    toks, feats = pieces[0].shape
    chunk = toks * len(pieces)
    group = QKV_GROUP
    wide = group * 3 * hd
    hbm = pl.BlockSpec(memory_space=pl.ANY)
    out_h = pl.BlockSpec((group, chunk, hd), lambda n, s: (n, 0, 0))
    out_i = pl.BlockSpec((chunk * heads, hd), lambda n, s: (0, 0))
    h_t = jax.ShapeDtypeStruct((heads, chunk, hd), BF16)
    i_t = jax.ShapeDtypeStruct((chunk * heads, hd), BF16)
    return pl.pallas_call(
        functools.partial(qkv_kernel, heads, hd, group),
        grid_spec=pltpu.PrefetchScalarGridSpec(
            num_scalar_prefetch=1,
            grid=(heads // group,),
            in_specs=[hbm] * 4 + [pl.BlockSpec((feats, wide), lambda n, s: (0, n)), pl.BlockSpec(b.shape, lambda n, s: (0,))],
            out_specs=[out_h, out_h, out_h, out_i, out_i],
            scratch_shapes=[pltpu.VMEM((chunk, feats), BF16)] + [pltpu.VMEM((chunk * heads, hd), F32)] * 2 + [pltpu.SemaphoreType.DMA((4,))],
        ),
        out_shape=[h_t, h_t, h_t, i_t, i_t],
        compiler_params=pltpu.CompilerParams(vmem_limit_bytes=VMEM_BIG),
        cost_estimate=pl.CostEstimate(flops=2 * chunk * feats * w.shape[1], bytes_accessed=w.size * 2 + chunk * feats * 2, transcendentals=0),
        name="qkv",
    )(idx, *pieces, w, b)


def attn_kernel(place, heads, idx_ref, len_ref, slope_ref, q_ref, kn_ref, vn_ref, kt_ref, vt_ref, ki_ref, vi_ref, kc_ref, vc_ref, *refs):
    c0, c1, c2, c3, ko_ref, vo_ref, m_s, l_s, acc_s, through, sems, isems, osems = refs[2 * (place > 0):]
    head = pl.program_id(0)
    seq = idx_ref[2 + place]
    length = len_ref[seq]
    chunk, hd = q_ref.shape[1], q_ref.shape[2]

    def old_in(n):
        return pltpu.make_async_copy((kc_ref, vc_ref)[n].at[seq], through.at[n], isems.at[n])

    def rows_in(n):
        return pltpu.make_async_copy((ki_ref, vi_ref)[n], through.at[n, pl.ds(length, chunk)], sems.at[n])

    def all_out(n):
        return pltpu.make_async_copy(through.at[n], (ko_ref, vo_ref)[n].at[seq], osems.at[n])

    @pl.when(head == 0)
    def _():
        for n in range(2):
            old_in(n).start()

    @pl.when(head == 1)
    def _():
        for n in range(2):
            old_in(n).wait()
            rows_in(n).start()

    @pl.when(head == 2)
    def _():
        for n in range(2):
            rows_in(n).wait()
            all_out(n).start()

    scale = LOG2E * hd ** -0.5
    slope = slope_ref[head] * LOG2E
    n_full = length // KB
    rest = length - n_full * KB
    tok = chunk // 4
    halves = range(chunk // QB)

    def scores(qi, k, base, rows=slice(0, QB)):
        q = q_ref[0, qi * QB + rows.start:qi * QB + rows.stop, :]
        s = lax.dot_general(q, k, (((1,), (1,)), ((), ())), preferred_element_type=F32) * scale
        pos = (lax.broadcasted_iota(jnp.int32, (1, k.shape[0]), 1) + (base - qi * QB)).astype(F32) * slope
        return s + pos

    def lanes_sum(p):
        tot = p[:, :128]
        for n in range(1, p.shape[1] // 128):
            tot = tot + p[:, n * 128:(n + 1) * 128]
        return tot

    def update(qi, s, v):
        m_prev = m_s[qi]
        m_new = jnp.maximum(m_prev, jnp.max(s, axis=1, keepdims=True))
        alpha = jnp.exp2(m_prev - m_new)
        p = jnp.exp2(s - jnp.tile(m_new, (1, KB // 128)))
        l_s[qi] = l_s[qi] * alpha + lanes_sum(p)
        acc_s[qi] = acc_s[qi] * alpha + jnp.dot(p.astype(BF16), v, preferred_element_type=F32)
        m_s[qi] = m_new

    for qi in halves:
        new = slice(qi * QB, (qi + 1) * QB)
        s = scores(qi, kn_ref[0, new, :], qi * QB)
        row = lax.broadcasted_iota(jnp.int32, (QB, KB), 0)
        col = lax.broadcasted_iota(jnp.int32, (QB, KB), 1)
        s = jnp.where(col <= row, s, MASKED)
        m_new = jnp.broadcast_to(jnp.max(s, axis=1, keepdims=True), (QB, 128))
        p = jnp.exp2(s - jnp.tile(m_new, (1, KB // 128)))
        m_s[qi] = m_new
        l_s[qi] = lanes_sum(p)
        acc_s[qi] = jnp.dot(p.astype(BF16), vn_ref[0, new, :], preferred_element_type=F32)

    for qi in halves:
        for kj in range(qi):
            blk = slice(kj * KB, (kj + 1) * KB)
            update(qi, scores(qi, kn_ref[0, blk, :], kj * KB), vn_ref[0, blk, :])

    def old_block(n, carry):
        start = pl.multiple_of(n * KB, KB)
        k, v = kt_ref[0, 0, pl.ds(start, KB), :], vt_ref[0, 0, pl.ds(start, KB), :]
        s = [scores(qi, k, start - length) for qi in halves]
        for qi in halves:
            update(qi, s[qi], v)
        return carry

    lax.fori_loop(0, n_full, old_block, 0)

    @pl.when(rest > 0)
    def _():
        start = pl.multiple_of(n_full * KB, KB)
        k, v = kt_ref[0, 0, pl.ds(start, KB), :], vt_ref[0, 0, pl.ds(start, KB), :]
        inside = lax.broadcasted_iota(jnp.int32, (QB, KB), 1) < rest
        for qi in halves:
            update(qi, jnp.where(inside, scores(qi, k, start - length), MASKED), v)

    for qi in halves:
        ctx = (acc_s[qi] / jnp.sum(l_s[qi], axis=1, keepdims=True)).astype(BF16)
        for j in range(QB // tok):
            owner = idx_ref[0] ^ (qi * (QB // tok) + j)
            for n, out in enumerate((c0, c1, c2, c3)):
                @pl.when(owner == n)
                def _(out=out, j=j, ctx=ctx):
                    out[...] = ctx[j * tok:(j + 1) * tok, :]

    @pl.when(head == heads - 1)
    def _():
        for n in range(2):
            all_out(n).wait()


def attend(place, idx, lens, slopes, q, kn, vn, kt, vt, ki, vi, kc, vc, outs):
    heads, chunk, hd = q.shape
    toks = kt.shape[2]
    tok = chunk // 4
    per_head = pl.BlockSpec((1, chunk, hd), lambda h, *_: (h, 0, 0))
    old = pl.BlockSpec((1, 1, toks, hd), lambda h, s, *_: (s[2 + place], h, 0, 0))
    hbm = pl.BlockSpec(memory_space=pl.ANY)
    piece = pl.BlockSpec((tok, hd), lambda h, *_: (0, h))
    piece_t = jax.ShapeDtypeStruct((tok, heads * hd), BF16)
    cache_t = jax.ShapeDtypeStruct(kc.shape, BF16)
    pairs = heads * chunk * (toks // 2 + chunk // 2)
    return pl.pallas_call(
        functools.partial(attn_kernel, place, heads),
        grid_spec=pltpu.PrefetchScalarGridSpec(
            num_scalar_prefetch=3,
            grid=(heads,),
            in_specs=[per_head] * 3 + [old, old] + [hbm] * (4 + len(outs)),
            out_specs=[piece] * 4 + [hbm, hbm],
            scratch_shapes=[pltpu.VMEM((chunk // QB, QB, 128), F32), pltpu.VMEM((chunk // QB, QB, 128), F32), pltpu.VMEM((chunk // QB, QB, hd), F32), pltpu.VMEM((2, *kc.shape[1:]), BF16),
                            pltpu.SemaphoreType.DMA((2,)), pltpu.SemaphoreType.DMA((2,)), pltpu.SemaphoreType.DMA((2,))],
        ),
        out_shape=[piece_t] * 4 + [cache_t, cache_t],
        input_output_aliases={12: 4, 13: 5} if outs else {},
        compiler_params=pltpu.CompilerParams(vmem_limit_bytes=VMEM_BIG, has_side_effects=True),
        cost_estimate=pl.CostEstimate(flops=8 * pairs * hd, bytes_accessed=4 * heads * toks * hd, transcendentals=pairs),
        name="attend",
    )(idx, lens, slopes, q, kn, vn, kt, vt, ki, vi, kc, vc, *outs)


def out_kernel(seqs, *refs):
    refs = list(refs)
    take = lambda n: [refs.pop(0) for _ in range(n)]
    (idx_ref,) = take(1)
    xs, ctx = take(1)[0], [take(4) for _ in seqs]
    near, far = take(2), [take(4), take(4)]
    b_ref, g_ref, lb_ref, r_ref, n_ref, xb, cb, wb, acc, xsem, csem, wsem = refs
    tok = ctx[0][0].shape[0]
    part = near[0].shape[0]
    few = part // 4
    copies = [pltpu.make_async_copy(xs.at[idx_ref[2 + n]], xb.at[i], xsem.at[i]) for i, n in enumerate(seqs)]
    for i in range(len(seqs)):
        for k in range(4):
            copies.append(pltpu.make_async_copy(ctx[i][k], cb.at[i * tok:(i + 1) * tok, k * part:(k + 1) * part], csem.at[i, k]))
    first_w = len(copies)
    parts = [[pltpu.make_async_copy(near[a], wb.at[a * part:(a + 1) * part], wsem.at[a, 0])] for a in range(2)]
    for a in range(2):
        parts.append([])
        for n in range(4):
            at = pl.ds(pl.multiple_of((a + 2) * part + (idx_ref[1] ^ n) * few, few), few)
            parts[-1].append(pltpu.make_async_copy(far[a][n], wb.at[at], wsem.at[a + 2, n]))
    copies += [c for group in parts for c in group]
    for copy in copies:
        copy.start()
    for copy in copies[:first_w]:
        copy.wait()
    for k in range(4):
        for copy in parts[k]:
            copy.wait()
        total = jnp.dot(cb[:, k * part:(k + 1) * part], wb[k * part:(k + 1) * part, :], preferred_element_type=F32)
        acc[...] = total if k == 0 else acc[...] + total
    for i in range(len(seqs)):
        rows = slice(i * tok, (i + 1) * tok)
        res = (xb[i].astype(F32) + acc[rows, :] + row_of(b_ref)).astype(BF16)
        r_ref[rows, :] = res
        n_ref[rows, :] = ln_rows(res, row_of(g_ref), row_of(lb_ref))


def out_proj(idx, x, seqs, ctx, near, far, b, g, lb):
    tok, feats = x.shape[1:]
    rows = tok * len(seqs)
    flat = [c for got in ctx for c in got]
    vec = pl.BlockSpec(b.shape, lambda n, s: (0,))
    hbm = pl.BlockSpec(memory_space=pl.ANY)
    t = jax.ShapeDtypeStruct((rows, feats), BF16)
    out = pl.BlockSpec((rows, feats), lambda n, s: (0, 0))
    return pl.pallas_call(
        functools.partial(out_kernel, seqs),
        grid_spec=pltpu.PrefetchScalarGridSpec(
            num_scalar_prefetch=1, grid=(1,),
            in_specs=[hbm] * (1 + len(flat) + 10) + [vec] * 3, out_specs=[out, out],
            scratch_shapes=[pltpu.VMEM((len(seqs), tok, feats), BF16), pltpu.VMEM((rows, feats), BF16), pltpu.VMEM((feats, feats), BF16),
                            pltpu.VMEM((rows, feats), F32), pltpu.SemaphoreType.DMA((len(seqs),)), pltpu.SemaphoreType.DMA((len(seqs), 4)), pltpu.SemaphoreType.DMA((4, 4))],
        ),
        out_shape=[t, t],
        compiler_params=pltpu.CompilerParams(vmem_limit_bytes=VMEM_BIG),
        cost_estimate=pl.CostEstimate(flops=2 * rows * feats * feats, bytes_accessed=2 * feats * feats, transcendentals=0),
        name="outp",
    )(idx, x, *flat, *near, *far[0], *far[1], b, g, lb)


def mlp_kernel(near, final, n_steps, groups, n_acc, bias_row, *refs):
    refs = list(refs)
    take = lambda n: [refs.pop(0) for _ in range(n)]
    (idx_ref,) = take(1)
    norms = take(groups)
    bias_refs = take(2) if near else None
    n_arr = 2 if near else 2 * n_steps
    ups, uqs, downs = take(n_arr), [] if near else take(n_arr), take(n_arr)
    acc_in = take(n_acc)
    res, bd_ref = (take(groups), take(1)[0]) if final else (None, None)
    (out,) = take(1)
    nb, rb, acc, ubuf, dbuf, bbuf, nsem, rsem, asem, usem, dsem, bsem = refs
    step = pl.program_id(0)
    feats, width = ubuf.shape[2:]
    half = acc.shape[0] if acc.shape[0] <= MLP_ROWS else acc.shape[0] // 2

    def piece_copies(i, a):
        slot = i % 2
        if near:
            cols = slice(i * width, (i + 1) * width)
            return [pltpu.make_async_copy(downs[a].at[cols, :], dbuf.at[slot, a * width:(a + 1) * width], dsem.at[slot, a]),
                    pltpu.make_async_copy(ups[a].at[:, cols], ubuf.at[slot, a], usem.at[slot, a, 0])]
        copies = [pltpu.make_async_copy(downs[n_steps * a + i], dbuf.at[slot, a * width:(a + 1) * width], dsem.at[slot, a])]
        for n, arrays in enumerate((ups, uqs)):
            piece, cols = arrays[n_steps * a + i], slice(n * width // 2, (n + 1) * width // 2)
            copies.append(pltpu.make_async_copy(piece.at[:feats], ubuf.at[slot, a, :, cols], usem.at[slot, a, n]))
            copies.append(pltpu.make_async_copy(piece.at[bias_row:bias_row + 16], bbuf.at[slot, a, :, cols], bsem.at[slot, a, n]))
        return copies

    def rows_of(arrays, dst, sem):
        at, copies = 0, []
        for n, a in enumerate(arrays):
            copies.append(pltpu.make_async_copy(a, dst.at[at:at + a.shape[0]], sem.at[n]))
            at += a.shape[0]
        return copies

    def await_at(i, which):
        @pl.when(step == i)
        def _():
            for copy in which(i):
                copy.wait()

    @pl.when(step == 0)
    def _():
        for copy in rows_of(norms, nb, nsem) + [c for a in range(2) for c in piece_copies(0, a)]:
            copy.start()
        if near:
            acc[...] = jnp.zeros_like(acc)
        else:
            for copy in rows_of(acc_in, acc, asem) + (rows_of(res, rb, rsem) if final else []):
                copy.start()
        for copy in rows_of(norms, nb, nsem):
            copy.wait()

    for i in range(1, n_steps):
        @pl.when(step + 1 == i)
        def _(i=i):
            for copy in [c for a in range(2) for c in piece_copies(i, a)]:
                copy.start()

    slot = lax.rem(step, 2)
    for n in range(acc.shape[0] // half):
        rows = slice(n * half, (n + 1) * half)
        acts = []
        for a in range(2):
            if n == 0:
                for i in range(n_steps):
                    await_at(i, lambda i, a=a: piece_copies(i, a)[1:])
            bias = row_of(bias_refs[a], pl.ds(pl.multiple_of(step * width, width), width)) if near else bbuf[slot, a][:1, :].astype(F32)
            pre = jnp.dot(nb[rows, :], ubuf[slot, a], preferred_element_type=F32) + bias
            acts.append(jax.nn.gelu(pre, approximate=True).astype(BF16))
        if n == 0:
            for i in range(n_steps):
                await_at(i, lambda i: piece_copies(i, 0)[:1] + piece_copies(i, 1)[:1])
            if not near:
                await_at(0, lambda i: rows_of(acc_in, acc, asem))
        acc[rows, :] += jnp.dot(jnp.concatenate(acts, axis=1), dbuf[slot], preferred_element_type=F32)

    @pl.when(step == n_steps - 1)
    def _():
        if not final:
            copy = pltpu.make_async_copy(acc, out, asem.at[0])
            copy.start()
            copy.wait()
        else:
            for copy in rows_of(res, rb, rsem):
                copy.wait()
            tok = out.shape[1]
            for n in range(out.shape[0]):
                rows = slice(n * tok, (n + 1) * tok)
                out[idx_ref[2 + n]] = (rb[rows, :].astype(F32) + acc[rows, :] + row_of(bd_ref)).astype(BF16)


def mlp(idx, norms, bias, ups, downs, width, seqs, acc=(), res=None, bd=None, bias_row=None):
    feats = norms[0].shape[1]
    rows = sum(a.shape[0] for a in norms)
    whole = lambda a: pl.BlockSpec(a.shape, lambda n, s: (0,) * len(a.shape))
    hbm = pl.BlockSpec(memory_space=pl.ANY)
    near, final = bias is not None, res is not None
    uqs = ()
    if not near:
        ups, uqs = ups
    n_steps = 4 if near else len(ups) // 2
    args = [*norms, *(bias if near else ()), *ups, *uqs, *downs, *acc]
    specs = [hbm] * len(norms) + [whole(v) for v in bias or ()] + [hbm] * (len(ups) + len(uqs) + len(downs) + len(acc))
    if final:
        args += [*res, bd]
        specs += [hbm] * len(res) + [whole(bd)]
        out_t = jax.ShapeDtypeStruct((seqs, rows // seqs, feats), BF16)
        out_spec = whole(out_t)
    else:
        out_t, out_spec = jax.ShapeDtypeStruct((rows, feats), F32), hbm
    return pl.pallas_call(
        functools.partial(mlp_kernel, near, final, n_steps, len(norms), len(acc), bias_row),
        grid_spec=pltpu.PrefetchScalarGridSpec(
            num_scalar_prefetch=1, grid=(n_steps,), in_specs=specs, out_specs=out_spec,
            scratch_shapes=[pltpu.VMEM((rows, feats), BF16), pltpu.VMEM((rows if final else 16, feats), BF16), pltpu.VMEM((rows, feats), F32), pltpu.VMEM((2, 2, feats, width), BF16),
                        pltpu.VMEM((2, 2 * width, feats), BF16), pltpu.VMEM((2, 2, 16, width), BF16), pltpu.SemaphoreType.DMA((len(norms),)), pltpu.SemaphoreType.DMA((len(norms),)),
                        pltpu.SemaphoreType.DMA((len(norms),)), pltpu.SemaphoreType.DMA((2, 2, 2)), pltpu.SemaphoreType.DMA((2, 2)), pltpu.SemaphoreType.DMA((2, 2, 2))],
        ),
        out_shape=out_t,
        compiler_params=pltpu.CompilerParams(vmem_limit_bytes=VMEM_BIG),
        cost_estimate=pl.CostEstimate(flops=8 * rows * feats * n_steps * width, bytes_accessed=8 * feats * n_steps * width, transcendentals=0),
        name="mlp",
    )(idx, *args)


def solution(mesh):
    tp_size, dp_size = mesh.shape['tp'], mesh.shape['dp']
    assert tp_size == 4 and dp_size == 4

    def tp_swap(a, k):
        return lax.ppermute(a, 'tp', [(i, i ^ k) for i in range(tp_size)])

    def dp_swap(a, k):
        return lax.ppermute(a, 'dp', [(i, i ^ k) for i in range(dp_size)])

    def local_layer(x_local, prefix_len, k_cache, v_cache, ln1_gain, ln1_bias, w_qkv, b_qkv, w_out, b_out, ln2_gain, ln2_bias, w_up, b_up, w_down, b_down):
        seqs, tok, feats = x_local.shape
        cache_len, heads, hd = k_cache.shape[1:]
        tp, dp = lax.axis_index('tp'), lax.axis_index('dp')
        before = (prefix_len[None, :] > prefix_len[:, None]) | ((prefix_len[None, :] == prefix_len[:, None]) & (jnp.arange(seqs)[None, :] < jnp.arange(seqs)[:, None]))
        rank = jnp.sum(before.astype(jnp.int32), axis=1)
        falling = jnp.sum(jnp.where(rank[None, :] == jnp.arange(seqs)[:, None], jnp.arange(seqs)[None, :], 0), axis=1)
        idx = jnp.concatenate([jnp.stack([tp, dp]), falling]).astype(jnp.int32)
        head_ids = tp * heads + jnp.arange(heads)
        slopes = jnp.exp2(-8.0 * (head_ids + 1).astype(F32) / (heads * tp_size))
        near_bias = [b_up, tp_swap(b_up, 1)]
        wo_s = tp_swap(w_out, 1)
        *normed, up_q, uq_q, down_q, wo_q = ln1(idx, x_local, ln1_gain, ln1_bias, b_up, w_up, w_down, w_out, dp_size)
        x_x = [tp_swap(normed[b], 2) for b in range(seqs)]
        x_s = [tp_swap(normed[b], 1) for b in range(seqs)]
        x_xs = [tp_swap(x_x[b], 1) for b in range(seqs)]

        width = w_up.shape[1] // dp_size

        def spread(piece, a, b, direct=False):
            first = tp_swap(piece, 2)
            one = dp_swap(first, a)
            two = dp_swap(first, b)
            both = dp_swap(first, 3) if direct else dp_swap(one, b)
            got = [first, one, two, both] if a == 1 else [first, two, one, both]
            return got, [tp_swap(a, 1) for a in got]

        up_x, up_xs = spread(up_q, 1, 2)
        uq_x, uq_xs = spread(uq_q, 1, 2, direct=True)
        down_x, down_xs = spread(down_q, 2, 1)
        wo_x, wo_xs = spread(wo_q, 1, 2)
        up_s, down_s = tp_swap(w_up, 1), tp_swap(w_down, 1)

        flat = (seqs, cache_len * heads, hd)
        kt, vt = prep(prefix_len, k_cache.reshape(flat), v_cache.reshape(flat), heads)
        caches = ()
        got = []
        inter = (tok * tp_size, heads, hd)
        for b in range(seqs):
            q, kn, vn, ki, vi = qkv(idx, [normed[b], x_s[b], x_x[b], x_xs[b]], w_qkv, b_qkv, heads, hd)
            *ctx, ko, vo = attend(b, idx, prefix_len, slopes, q, kn, vn, kt, vt, ki.reshape(inter), vi.reshape(inter), k_cache, v_cache, caches)
            caches = (ko, vo)
            got.append([ctx[0]] + [tp_swap(ctx[k], k) for k in (1, 2, 3)])
        norms, resid = [], []
        for some in (tuple(range(seqs - 1)), (seqs - 1,)):
            r, n2 = out_proj(idx, x_local, some, [got[b] for b in some], [w_out, wo_s], [wo_x, wo_xs], b_out, ln2_gain, ln2_bias)
            resid.append(r)
            norms.append(n2)
        acc = mlp(idx, norms, near_bias, [w_up, up_s], [w_down, down_s], width, seqs)
        out = mlp(idx, norms, None, [up_x + up_xs, uq_x + uq_xs], down_x + down_xs, width, seqs, [acc], resid, b_down, feats)
        return out, ko, vo

    tok_spec = P('dp', 'tp', None)
    cache_spec = P('dp', None, 'tp', None)
    rep = P()
    in_specs = (tok_spec, P('dp'), cache_spec, cache_spec, rep, rep, P(None, 'tp'), P('tp'), P('tp', None), rep, rep, rep, P(None, 'tp'), P('tp'), P('tp', None), rep)
    return jax.shard_map(local_layer, mesh=mesh, in_specs=in_specs, out_specs=(tok_spec, cache_spec, cache_spec), check_vma=False)
```
